1024 devices in a mesh: curve: 64 (over y, x), lev: 16 (over z, core).
Axes of the slice: x: 8, y: 8, z: 8, core: 2. Of those that a mesh axis runs over, the one named last changes fastest.
Arguments:
- source_field: bfloat16 [1048576, 1024], P(('curve', 'lev')), may hold values from -6 to 6
- slot_elems: int32 [16, 131072], P(None, ('curve', 'lev')), may hold values from 0 to 1023
- slot_tiles: int32 [131072], P(('curve', 'lev')), may hold values from 0 to 16383, as said below
- weights: bfloat16 [131072, 16, 256], P(('curve', 'lev')), may hold values from -0.375 to 0.375
Outputs:
- remapped: float32 [64, 262144], P(None, ('curve', 'lev'))
The draws below stay inside these ranges and needn't reach their ends.
Inputs may be any that keep to these rules, and one draw needn't show every extreme that they name: `slot_elems`: local element ids within the slot's own device's elements. `slot_tiles`: tile g belongs to band g // 256. The 128 slots of a device with curve index b name tiles of the 4 bands b to b + 4 - 1 modulo 64 only, at most 64 of them in one band, a bound reached on every device, and exactly 2 tiles of each residue modulo 64.
All inputs are finite; a program needn't handle non-finite values.
Results may differ from the reference program's by a relative error of at most 0.0003.
Values sent between devices are 32-bit elements; how exact they have to be, the bound alone decides.
No kernel may reach another device: no remote copies, remote signals or barrier semaphores. Data moves between devices by JAX's collectives and lax.ppermute only.
A program may use at most 64 MiB of HBM per device.

```python
import jax
import jax.numpy as jnp
from jax import lax

CH = 64
NODE = 16
TILE = 16
EPB = 16
NB = 4
ELEM_DEV = 1024
ELEMS = 1048576
CELLS = 262144
TPBAND = 256
NTILE = 16384
PER = 4
LB = 128
SLOTS = 131072
N_CURVE = 64
N_LEV = 16


def draw_slot_tiles(key, part):
    count_key = jax.random.fold_in(key, 21)
    shift_key = jax.random.fold_in(key, 22)
    high_key = jax.random.fold_in(key, 23)
    order_key = jax.random.fold_in(key, 24)
    devices = N_CURVE * N_LEV
    counts = jnp.array([LB // 2, LB // 4, LB // 8, LB // 8], dtype=jnp.int32)
    count_order = jax.random.permutation(count_key, NB).astype(jnp.int32)
    device_ids = jnp.arange(devices, dtype=jnp.int32)
    curve_ids = device_ids // N_LEV
    band_steps = jnp.arange(NB, dtype=jnp.int32)
    per_band = counts[count_order[(curve_ids[:, None] + band_steps[None, :]) % NB]]
    band_ends = jnp.cumsum(per_band, axis=1)
    slot_index = jnp.arange(LB, dtype=jnp.int32)
    offset = jnp.sum((slot_index[None, :, None] >= band_ends[:, None, :]).astype(jnp.int32), axis=2)
    band_ids = (curve_ids[:, None] + offset) % N_CURVE
    rshift = jax.random.randint(shift_key, (devices, 1), 0, N_CURVE, dtype=jnp.int32)
    residue = (slot_index[None, :] + rshift) % N_CURVE
    high_part = jax.random.randint(high_key, (devices, LB), 0, PER, dtype=jnp.int32)
    tile_ids = band_ids * TPBAND + high_part * N_CURVE + residue

    def shuffle_order(device_key):
        return jax.random.permutation(device_key, LB)
    orders = jax.vmap(shuffle_order)(jax.random.split(order_key, devices))
    shuffled = jnp.take_along_axis(tile_ids, orders, axis=1)
    return shuffled.reshape(devices * LB).astype(jnp.int32)


def set_ends(entries, own_key, least, top_value):
    place = [jax.random.randint(jax.random.fold_in(own_key, axis), (), 0, length) for axis, length in enumerate(entries.shape)]
    widest = entries.shape.index(max(entries.shape))
    next_to = place[:widest] + [(place[widest] + 1) % entries.shape[widest]] + place[widest + 1:]
    return entries.at[tuple(place)].set(least).at[tuple(next_to)].set(top_value)


def block_scale(key, dims, cuts, least, largest):
    level, own = 1.0, jax.random.fold_in(key, 6)
    for axis_at, blocks in cuts:
        steps = jnp.exp(jax.random.uniform(jax.random.fold_in(own, axis_at), (blocks,), jnp.float32, least / len(cuts), largest / len(cuts)))
        level = level * jnp.repeat(steps, dims[axis_at] // blocks).reshape([-1 if axis == axis_at else 1 for axis in range(len(dims))])
    return level


def bell_draw(own_key, dims, scale, limit, cuts=(), kind=jnp.bfloat16):
    values = jax.random.normal(own_key, dims, jnp.float32) * scale
    if len(cuts) > 0:
        values = block_scale(own_key, dims, cuts, -0.22, 0.18) * values
    return jnp.clip(values, min=-limit, max=limit).astype(kind)


def setup_inputs(seed: int = 0) -> dict:
    key_of = jax.random.split(jax.random.key(seed), 5)
    source_field = bell_draw(key_of[0], (ELEMS, NODE * CH), 1.0, 6.0, ((0, 1024),))
    slot_elems = set_ends(jax.random.randint(key_of[1], (EPB, SLOTS), 0, ELEM_DEV), jax.random.fold_in(key_of[1], 1), 0, ELEM_DEV - 1).astype(jnp.int32)
    slot_tiles = draw_slot_tiles(jax.random.fold_in(key_of[4], 71), 0)
    weights = bell_draw(key_of[3], (SLOTS, TILE, EPB * NODE), (EPB * NODE) ** -0.5, 0.375, ((0, 1024),))
    return {"source_field": source_field, "slot_elems": slot_elems, "slot_tiles": slot_tiles, "weights": weights}


def reference(source_field, slot_elems, slot_tiles, weights):
    devices = N_CURVE * N_LEV
    row_width = CH * TILE

    def one_device(grid_total, device):
        segment = lax.dynamic_slice_in_dim(source_field, (device * ELEM_DEV).astype(jnp.int32), ELEM_DEV, 0)
        element_ids = lax.dynamic_slice_in_dim(slot_elems, (device * LB).astype(jnp.int32), LB, 1)
        gathered = jnp.take(segment, jnp.transpose(element_ids), axis=0)
        values = gathered.reshape(LB, EPB * NODE, CH)
        slot_weights = lax.dynamic_slice_in_dim(weights, (device * LB).astype(jnp.int32), LB, 0)
        partial_value = jnp.einsum("jnc,jtn->jct", values.astype(jnp.float32), slot_weights.astype(jnp.float32))
        slot_tile_ids = lax.dynamic_slice_in_dim(slot_tiles, (device * LB).astype(jnp.int32), LB, 0)
        grid_total = grid_total.at[slot_tile_ids].add(partial_value.reshape(LB, row_width))
        return grid_total, None

    start_total = jnp.zeros((NTILE, row_width), jnp.float32)
    grid_total, unused = lax.scan(one_device, start_total, jnp.arange(devices, dtype=jnp.int32))
    return jnp.transpose(grid_total.reshape(NTILE, CH, TILE), (1, 0, 2)).reshape(CH, CELLS)
```

```python
import jax
import jax.numpy as jnp
from jax import lax
from jax.experimental import pallas as pl
from jax.experimental.pallas import tpu as pltpu
from jax.sharding import PartitionSpec as P

NB = 4
LANES = 128
RESIDUES = 64
CLASSES = 4
PEERS = 16
CHUNK = 65
PIECES = 4
UNROLL = 32


def partials_kernel(
    elems, tiles, source, weights, out, nodes, regrouped, named, bf_source, bf_weights, row_of, sems
):
    band_index = lax.axis_index("curve")
    weights_in = pltpu.make_async_copy(weights, bf_weights, sems.at[PIECES])
    weights_in.start()
    rows_each = 1024 // PIECES
    source_in = []
    for k in range(PIECES):
        part = pl.ds(k * rows_each, rows_each)
        source_in.append(pltpu.make_async_copy(source.at[part], bf_source.at[part], sems.at[k]))
        source_in[k].start()

    for residue in range(RESIDUES):
        peer = ((residue >> 2) & 3) * CLASSES + (residue >> 4)
        row_of[residue] = peer * CHUNK + (residue & 3) * 16

    old = lax.broadcasted_iota(jnp.int32, (256, 256), 0)
    new = lax.broadcasted_iota(jnp.int32, (256, 256), 1)
    wanted = ((new >> 3) & 15) * 16 + (new & 7) * 2 + (new >> 7)
    reorder = jnp.where(old == wanted, 1.0, 0.0).astype(jnp.bfloat16)
    weights_in.wait()

    def regroup(i, carry):
        at = pl.ds(i * 32, 32)
        moved = jnp.dot(bf_weights[at].reshape(512, 256), reorder, preferred_element_type=jnp.float32)
        moved = moved.astype(jnp.bfloat16)
        regrouped[at, 0] = moved[:, :LANES].reshape(32, 16, LANES)
        regrouped[at, 1] = moved[:, LANES:].reshape(32, 16, LANES)
        return carry

    lax.fori_loop(0, 4, regroup, 0)

    def unfold(i, carry):
        for half in range(2):
            at = i * 2 + half
            block = bf_source[pl.ds(pl.multiple_of(at * 16, 16), 16), :].astype(jnp.float32)
            for pair in range(8):
                nodes[pl.ds(at * 128 + pair, 16, stride=8), :] = block[
                    :, pair * LANES : (pair + 1) * LANES
                ]
        return carry

    for k in range(PIECES):
        source_in[k].wait()
        lax.fori_loop(k * rows_each // 32, (k + 1) * rows_each // 32, unfold, 0)

    low_half = lax.broadcasted_iota(jnp.int32, (8, LANES), 1) < 64

    def one_slot(s):
        rows = [
            nodes[pl.ds(pl.multiple_of(elems[e * 128 + s] * 8, 8), 8), :] for e in range(16)
        ]
        values = jnp.concatenate(rows, axis=0).astype(jnp.bfloat16)
        product = jnp.dot(
            regrouped[s].reshape(32, LANES), values, preferred_element_type=jnp.float32
        )
        first, second, third, fourth = (product[8 * k : 8 * k + 8] for k in range(4))
        straight = jnp.where(low_half, first, fourth)
        crossed = jnp.where(low_half, second, third)
        partial = straight + pltpu.roll(crossed, 64, 1)
        tile = tiles[s]
        residue = tile & 63
        row = row_of[residue]
        row_of[residue] = row + 8
        out[pl.ds(row, 8), :] = partial
        named[pl.ds(row >> 3, 1), :] = jnp.full((1, LANES), tile, jnp.int32)

    def slots(i, carry):
        for k in range(UNROLL):
            one_slot(i * UNROLL + k)
        return carry

    lax.fori_loop(0, 128 // UNROLL, slots, 0)

    diagonal = lax.broadcasted_iota(jnp.int32, (8, LANES), 0) == lax.broadcasted_iota(
        jnp.int32, (8, LANES), 1
    )
    for peer in range(PEERS):
        tags = (named[pl.ds(peer * 8 + (peer >> 3), 8), :] - band_index * 256) & 1023
        tags = ((tags >> 6) << 2) | (tags & 3)
        tags = jnp.where(diagonal, tags.astype(jnp.float32), 0.0)
        out[pl.ds(peer * CHUNK + 64, 1), :] = jnp.sum(tags, axis=0, keepdims=True)


def bins_kernel(arrived, *outs):
    diagonal = lax.broadcasted_iota(jnp.int32, (8, LANES), 0) == lax.broadcasted_iota(
        jnp.int32, (8, LANES), 1
    )
    bin_ids = lax.broadcasted_iota(jnp.int32, (8, LANES), 1).astype(jnp.float32)
    chosen = []
    for peer in range(PEERS):
        tags = jnp.where(diagonal, arrived[pl.ds(peer * CHUNK + 64, 8, stride=0), :], 0.0)
        chosen.append(jnp.where(jnp.sum(tags, axis=1, keepdims=True) == bin_ids, 1.0, 0.0))
    chosen = jnp.transpose(jnp.concatenate(chosen, axis=0))[:64].astype(jnp.bfloat16)
    for i in range(8):
        exact = jnp.concatenate(
            [arrived[pl.ds(peer * CHUNK + i, 8, stride=8), :] for peer in range(PEERS)], axis=0
        )
        high = exact.astype(jnp.bfloat16)
        rest = exact - high.astype(jnp.float32)
        middle = rest.astype(jnp.bfloat16)
        low = (rest - middle.astype(jnp.float32)).astype(jnp.bfloat16)
        total = sum(
            jnp.dot(chosen, part, preferred_element_type=jnp.float32) for part in (low, middle, high)
        )
        for step in range(NB):
            outs[step][pl.ds(i, 16, stride=8), :] = total[16 * step : 16 * step + 16]


def boxes_kernel(tiles, out):
    for half in range(2):
        rows = []
        for k in range(8):
            tile = tiles[pl.ds((half * 8 + k) * 8, 8), :]
            rows += [tile, pltpu.roll(tile, 64, 1)]
        turned = jnp.transpose(jnp.concatenate(rows, axis=0))
        out[:, half * LANES : (half + 1) * LANES] = turned[:64]


def in_vmem():
    return pl.BlockSpec(memory_space=pltpu.VMEM)


def budget(mib):
    return pltpu.CompilerParams(vmem_limit_bytes=mib * 2**20)


def partials(slot_elems, slot_tiles, source_field, weights):
    scalars = pl.BlockSpec(memory_space=pltpu.SMEM)
    outside = pl.BlockSpec(memory_space=pltpu.HBM)
    return pl.pallas_call(
        partials_kernel,
        out_shape=jax.ShapeDtypeStruct((PEERS * CHUNK, LANES), jnp.float32),
        in_specs=[scalars, scalars, outside, outside],
        out_specs=in_vmem(),
        scratch_shapes=[
            pltpu.VMEM((8192, LANES), jnp.float32),
            pltpu.VMEM((128, 2, 16, LANES), jnp.bfloat16),
            pltpu.VMEM((136, LANES), jnp.int32),
            pltpu.VMEM((1024, 1024), jnp.bfloat16),
            pltpu.VMEM((128, 16, 256), jnp.bfloat16),
            pltpu.SMEM((RESIDUES,), jnp.int32),
            pltpu.SemaphoreType.DMA((PIECES + 1,)),
        ],
        compiler_params=budget(53),
        name="partials",
    )(slot_elems.reshape(-1), slot_tiles, source_field, weights)


def bins(arrived):
    return pl.pallas_call(
        bins_kernel,
        out_shape=[jax.ShapeDtypeStruct((LANES, LANES), jnp.float32)] * NB,
        in_specs=[in_vmem()],
        out_specs=[in_vmem()] * NB,
        compiler_params=budget(8),
        name="bins",
    )(arrived)


def boxes(tiles):
    return pl.pallas_call(
        boxes_kernel,
        out_shape=jax.ShapeDtypeStruct((64, 256), jnp.float32),
        in_specs=[in_vmem()],
        out_specs=in_vmem(),
        compiler_params=budget(4),
        name="boxes",
    )(tiles)


def per_device(source_field, slot_elems, slot_tiles, weights):
    curve_size = lax.axis_size("curve")
    lev_size = lax.axis_size("lev")
    sending = partials(slot_elems, slot_tiles, source_field, weights)
    arrived = lax.all_to_all(
        sending.reshape(lev_size, 1, CHUNK * LANES), "lev", split_axis=0, concat_axis=0, tiled=True
    )
    steps = bins(arrived.reshape(PEERS * CHUNK, LANES))
    total = steps[0]
    for step in range(NB - 1, 0, -1):
        route = [(i, (i + step) % curve_size) for i in range(curve_size)]
        total = total + lax.ppermute(steps[step], "curve", route)
    groups = [[c + CLASSES * k for k in range(lev_size // CLASSES)] for c in range(CLASSES)]
    mine = lax.all_to_all(
        total.reshape(4, 32, LANES),
        "lev",
        split_axis=0,
        concat_axis=0,
        tiled=True,
        axis_index_groups=groups,
    )
    return boxes(mine.reshape(LANES, LANES))


def solution(mesh):
    placed = (
        P(("curve", "lev"), None),
        P(None, ("curve", "lev")),
        P(("curve", "lev")),
        P(("curve", "lev"), None, None),
    )
    return jax.shard_map(
        per_device, mesh=mesh, in_specs=placed, out_specs=P(None, ("curve", "lev")), check_vma=False
    )
```

```python
import jax
import jax.numpy as jnp
from jax import lax
from jax.experimental import pallas as pl
from jax.experimental.pallas import tpu as pltpu
from jax.sharding import PartitionSpec as P

NB = 4
LANES = 128
RESIDUES = 64
CLASSES = 4
PEERS = 16
CHUNK = 65
PIECES = 4


def partials_kernel(
    slot_elems,
    slot_tiles,
    source,
    weights,
    out,
    nodes,
    regrouped,
    named,
    bf_source,
    bf_weights,
    elems,
    elem_rows,
    tiles,
    row_of,
    sems,
):
    band_index = lax.axis_index("curve")
    scalars_in = [
        pltpu.make_async_copy(slot_elems, elems, sems.at[PIECES + 1]),
        pltpu.make_async_copy(slot_tiles, tiles, sems.at[PIECES + 2]),
    ]
    for copy in scalars_in:
        copy.start()
    weights_in = pltpu.make_async_copy(weights, bf_weights, sems.at[PIECES])
    weights_in.start()
    rows_each = 1024 // PIECES
    source_in = []
    for k in range(PIECES):
        part = pl.ds(k * rows_each, rows_each)
        source_in.append(pltpu.make_async_copy(source.at[part], bf_source.at[part], sems.at[k]))
        source_in[k].start()

    for residue in range(RESIDUES):
        peer = ((residue >> 2) & 3) * CLASSES + (residue >> 4)
        row_of[residue] = peer * CHUNK + (residue & 3) * 16

    old = lax.broadcasted_iota(jnp.int32, (256, 256), 0)
    new = lax.broadcasted_iota(jnp.int32, (256, 256), 1)
    wanted = ((new >> 3) & 15) * 16 + (new & 7) * 2 + (new >> 7)
    reorder = jnp.where(old == wanted, 1.0, 0.0).astype(jnp.bfloat16)
    weights_in.wait()

    def regroup(i, carry):
        at = pl.ds(i * 32, 32)
        moved = jnp.dot(bf_weights[at].reshape(512, 256), reorder, preferred_element_type=jnp.float32)
        moved = moved.astype(jnp.bfloat16)
        regrouped[at, 0] = moved[:, :LANES].reshape(32, 16, LANES)
        regrouped[at, 1] = moved[:, LANES:].reshape(32, 16, LANES)
        return carry

    lax.fori_loop(0, 4, regroup, 0)

    scalars_in[0].wait()
    elems[...] = elems[...] * 8
    scaled_in = pltpu.make_async_copy(elems, elem_rows, sems.at[PIECES + 3])
    scaled_in.start()

    def unfold(i, carry):
        for half in range(2):
            at = i * 2 + half
            block = bf_source[pl.ds(pl.multiple_of(at * 16, 16), 16), :].astype(jnp.float32)
            for pair in range(8):
                nodes[pl.ds(at * 128 + pair, 16, stride=8), :] = block[
                    :, pair * LANES : (pair + 1) * LANES
                ]
        return carry

    for k in range(PIECES):
        source_in[k].wait()
        lax.fori_loop(k * rows_each // 32, (k + 1) * rows_each // 32, unfold, 0)

    scaled_in.wait()
    scalars_in[1].wait()
    low_half = lax.broadcasted_iota(jnp.int32, (8, LANES), 1) < 64

    def one_slot(s):
        rows = [
            nodes[pl.ds(pl.multiple_of(elem_rows[e, s], 8), 8), :] for e in range(16)
        ]
        values = jnp.concatenate(rows, axis=0).astype(jnp.bfloat16)
        product = jnp.dot(
            regrouped[s].reshape(32, LANES), values, preferred_element_type=jnp.float32
        )
        first, second, third, fourth = (product[8 * k : 8 * k + 8] for k in range(4))
        straight = jnp.where(low_half, first, fourth)
        crossed = jnp.where(low_half, second, third)
        partial = straight + pltpu.roll(crossed, 64, 1)
        tile = tiles[s]
        residue = tile & 63
        row = row_of[residue]
        row_of[residue] = row + 8
        out[pl.ds(row, 8), :] = partial
        named[pl.ds(row >> 3, 1), :] = jnp.full((1, LANES), tile, jnp.int32)

    for s in range(128):
        one_slot(s)

    diagonal = lax.broadcasted_iota(jnp.int32, (8, LANES), 0) == lax.broadcasted_iota(
        jnp.int32, (8, LANES), 1
    )
    for peer in range(PEERS):
        tags = (named[pl.ds(peer * 8 + (peer >> 3), 8), :] - band_index * 256) & 1023
        tags = ((tags >> 6) << 2) | (tags & 3)
        tags = jnp.where(diagonal, tags.astype(jnp.float32), 0.0)
        out[pl.ds(peer * CHUNK + 64, 1), :] = jnp.sum(tags, axis=0, keepdims=True)


def bins_kernel(arrived, *outs):
    diagonal = lax.broadcasted_iota(jnp.int32, (8, LANES), 0) == lax.broadcasted_iota(
        jnp.int32, (8, LANES), 1
    )
    bin_ids = lax.broadcasted_iota(jnp.int32, (8, LANES), 1).astype(jnp.float32)
    chosen = []
    for peer in range(PEERS):
        tags = jnp.where(diagonal, arrived[pl.ds(peer * CHUNK + 64, 8, stride=0), :], 0.0)
        chosen.append(jnp.where(jnp.sum(tags, axis=1, keepdims=True) == bin_ids, 1.0, 0.0))
    chosen = jnp.transpose(jnp.concatenate(chosen, axis=0))[:64].astype(jnp.bfloat16)
    for i in range(8):
        exact = jnp.concatenate(
            [arrived[pl.ds(peer * CHUNK + i, 8, stride=8), :] for peer in range(PEERS)], axis=0
        )
        high = exact.astype(jnp.bfloat16)
        rest = exact - high.astype(jnp.float32)
        middle = rest.astype(jnp.bfloat16)
        low = (rest - middle.astype(jnp.float32)).astype(jnp.bfloat16)
        total = sum(
            jnp.dot(chosen, part, preferred_element_type=jnp.float32) for part in (low, middle, high)
        )
        for step in range(NB):
            outs[step & 1][pl.ds((step >> 1) * LANES + i, 16, stride=8), :] = total[
                16 * step : 16 * step + 16
            ]


def boxes_kernel(tiles, out):
    for half in range(2):
        rows = []
        for k in range(8):
            tile = tiles[pl.ds((half * 8 + k) * 8, 8), :]
            rows += [tile, pltpu.roll(tile, 64, 1)]
        turned = jnp.transpose(jnp.concatenate(rows, axis=0))
        out[:, half * LANES : (half + 1) * LANES] = turned[:64]


def in_vmem():
    return pl.BlockSpec(memory_space=pltpu.VMEM)


def budget(mib):
    return pltpu.CompilerParams(vmem_limit_bytes=mib * 2**20)


def partials(slot_elems, slot_tiles, source_field, weights):
    outside = pl.BlockSpec(memory_space=pltpu.HBM)
    return pl.pallas_call(
        partials_kernel,
        out_shape=jax.ShapeDtypeStruct((PEERS * CHUNK, LANES), jnp.float32),
        in_specs=[outside] * 4,
        out_specs=in_vmem(),
        scratch_shapes=[
            pltpu.VMEM((8192, LANES), jnp.float32),
            pltpu.VMEM((128, 2, 16, LANES), jnp.bfloat16),
            pltpu.VMEM((136, LANES), jnp.int32),
            pltpu.VMEM((1024, 1024), jnp.bfloat16),
            pltpu.VMEM((128, 16, 256), jnp.bfloat16),
            pltpu.VMEM((16, 128), jnp.int32),
            pltpu.SMEM((16, 128), jnp.int32),
            pltpu.SMEM((128,), jnp.int32),
            pltpu.SMEM((RESIDUES,), jnp.int32),
            pltpu.SemaphoreType.DMA((PIECES + 4,)),
        ],
        compiler_params=budget(53),
        name="partials",
    )(
        pltpu.with_memory_space_constraint(slot_elems, pltpu.HBM),
        pltpu.with_memory_space_constraint(slot_tiles, pltpu.HBM),
        source_field,
        weights,
    )


def bins(arrived):
    return pl.pallas_call(
        bins_kernel,
        out_shape=[jax.ShapeDtypeStruct((2 * LANES, LANES), jnp.float32)] * 2,
        in_specs=[in_vmem()],
        out_specs=[in_vmem()] * 2,
        compiler_params=budget(8),
        name="bins",
    )(arrived)


def boxes(tiles):
    return pl.pallas_call(
        boxes_kernel,
        out_shape=jax.ShapeDtypeStruct((64, 256), jnp.float32),
        in_specs=[in_vmem()],
        out_specs=in_vmem(),
        compiler_params=budget(4),
        name="boxes",
    )(tiles)


def ahead(block, distance):
    size = lax.axis_size("curve")
    return lax.ppermute(block, "curve", [(i, (i + distance) % size) for i in range(size)])


def per_device(source_field, slot_elems, slot_tiles, weights):
    lev_size = lax.axis_size("lev")
    sending = partials(slot_elems, slot_tiles, source_field, weights)
    arrived = lax.all_to_all(
        sending.reshape(lev_size, 1, CHUNK * LANES), "lev", split_axis=0, concat_axis=0, tiled=True
    )
    near, far = bins(arrived.reshape(PEERS * CHUNK, LANES))
    far = ahead(far, 1)
    total = near[:LANES] + far[:LANES] + ahead(near[LANES:] + far[LANES:], 2)
    groups = [[c + CLASSES * k for k in range(lev_size // CLASSES)] for c in range(CLASSES)]
    mine = lax.all_to_all(
        total.reshape(4, 32, LANES),
        "lev",
        split_axis=0,
        concat_axis=0,
        tiled=True,
        axis_index_groups=groups,
    )
    return boxes(mine.reshape(LANES, LANES))


def solution(mesh):
    placed = (
        P(("curve", "lev"), None),
        P(None, ("curve", "lev")),
        P(("curve", "lev")),
        P(("curve", "lev"), None, None),
    )
    return jax.shard_map(
        per_device, mesh=mesh, in_specs=placed, out_specs=P(None, ("curve", "lev")), check_vma=False
    )
```

```python
import jax
import jax.numpy as jnp
from jax import lax
from jax.experimental import pallas as pl
from jax.experimental.pallas import tpu as pltpu
from jax.sharding import PartitionSpec as P

LANES = 128
RESIDUES = 64
CLASSES = 4
PEERS = 32
CHUNK = 33
PIECES = 4


def partials_kernel(
    slot_elems,
    slot_tiles,
    source,
    weights,
    out,
    nodes,
    regrouped,
    named,
    bf_source,
    bf_weights,
    elems,
    elem_rows,
    tiles,
    row_of,
    sems,
):
    band_index = lax.axis_index("curve")
    scalars_in = [
        pltpu.make_async_copy(slot_elems, elems, sems.at[PIECES + 1]),
        pltpu.make_async_copy(slot_tiles, tiles, sems.at[PIECES + 2]),
    ]
    for copy in scalars_in:
        copy.start()
    weights_in = pltpu.make_async_copy(weights, bf_weights, sems.at[PIECES])
    weights_in.start()
    rows_each = 1024 // PIECES
    source_in = []
    for k in range(PIECES):
        part = pl.ds(k * rows_each, rows_each)
        source_in.append(pltpu.make_async_copy(source.at[part], bf_source.at[part], sems.at[k]))
        source_in[k].start()

    for residue in range(RESIDUES):
        peer = ((residue >> 1) & 1) * 16 + ((residue >> 2) & 3) * CLASSES + (residue >> 4)
        row_of[residue] = peer * CHUNK + (residue & 1) * 16

    old = lax.broadcasted_iota(jnp.int32, (256, 256), 0)
    new = lax.broadcasted_iota(jnp.int32, (256, 256), 1)
    wanted = ((new >> 3) & 15) * 16 + (new & 7) * 2 + (new >> 7)
    reorder = jnp.where(old == wanted, 1.0, 0.0).astype(jnp.bfloat16)
    weights_in.wait()

    def regroup(i, carry):
        at = pl.ds(i * 32, 32)
        moved = jnp.dot(bf_weights[at].reshape(512, 256), reorder, preferred_element_type=jnp.float32)
        moved = moved.astype(jnp.bfloat16)
        regrouped[at, 0] = moved[:, :LANES].reshape(32, 16, LANES)
        regrouped[at, 1] = moved[:, LANES:].reshape(32, 16, LANES)
        return carry

    lax.fori_loop(0, 4, regroup, 0)

    scalars_in[0].wait()
    elems[...] = elems[...] * 8
    scaled_in = pltpu.make_async_copy(elems, elem_rows, sems.at[PIECES + 3])
    scaled_in.start()

    def unfold(i, carry):
        for half in range(2):
            at = i * 2 + half
            block = bf_source[pl.ds(pl.multiple_of(at * 16, 16), 16), :].astype(jnp.float32)
            for pair in range(8):
                nodes[pl.ds(at * 128 + pair, 16, stride=8), :] = block[
                    :, pair * LANES : (pair + 1) * LANES
                ]
        return carry

    for k in range(PIECES):
        source_in[k].wait()
        lax.fori_loop(k * rows_each // 32, (k + 1) * rows_each // 32, unfold, 0)

    scaled_in.wait()
    scalars_in[1].wait()
    low_half = lax.broadcasted_iota(jnp.int32, (8, LANES), 1) < 64

    def one_slot(s):
        rows = [
            nodes[pl.ds(pl.multiple_of(elem_rows[e, s], 8), 8), :] for e in range(16)
        ]
        values = jnp.concatenate(rows, axis=0).astype(jnp.bfloat16)
        product = jnp.dot(
            regrouped[s].reshape(32, LANES), values, preferred_element_type=jnp.float32
        )
        first, second, third, fourth = (product[8 * k : 8 * k + 8] for k in range(4))
        straight = jnp.where(low_half, first, fourth)
        crossed = jnp.where(low_half, second, third)
        partial = straight + pltpu.roll(crossed, 64, 1)
        tile = tiles[s]
        residue = tile & 63
        row = row_of[residue]
        row_of[residue] = row + 8
        out[pl.ds(row, 8), :] = partial
        named[pl.ds(row >> 3, 1), :] = jnp.full((1, LANES), tile, jnp.int32)

    for s in range(128):
        one_slot(s)

    diagonal = lax.broadcasted_iota(jnp.int32, (4, LANES), 0) == lax.broadcasted_iota(
        jnp.int32, (4, LANES), 1
    )
    for peer in range(PEERS):
        tags = named[pl.ds(peer * 4 + (peer >> 3), 4), :] - (band_index >> 1) * 512
        tags = tags & 16383
        tags = ((tags >> 6) << 1) | (tags & 1)
        tags = jnp.where(diagonal, tags.astype(jnp.float32), 0.0)
        out[pl.ds(peer * CHUNK + 32, 1), :] = jnp.sum(tags, axis=0, keepdims=True)


def bins_kernel(arrived, own, second, third):
    lanes = lax.broadcasted_iota(jnp.int32, (PEERS, LANES), 1)
    bin_ids = lanes.astype(jnp.float32)
    named = arrived[pl.ds(32, PEERS, stride=CHUNK), :]
    chosen = []
    for place in range(4):
        tags = jnp.sum(jnp.where(lanes == place, named, 0.0), axis=1, keepdims=True)
        chosen.append(jnp.where(tags == bin_ids, 1.0, 0.0))
    chosen = jnp.transpose(jnp.concatenate(chosen, axis=0))[:40].astype(jnp.bfloat16)
    for i in range(8):
        exact = jnp.concatenate(
            [arrived[pl.ds(place * 8 + i, PEERS, stride=CHUNK), :] for place in range(4)], axis=0
        )
        high = exact.astype(jnp.bfloat16)
        rest = exact - high.astype(jnp.float32)
        middle = rest.astype(jnp.bfloat16)
        low = (rest - middle.astype(jnp.float32)).astype(jnp.bfloat16)
        total = sum(
            jnp.dot(chosen, part, preferred_element_type=jnp.float32) for part in (low, middle, high)
        )
        own[pl.ds(i, 16, stride=8), :] = total[:16]
        second[pl.ds(i, 16, stride=8), :] = total[16:32]
        third[pl.ds(i, 8, stride=8), :] = total[32:40]


def boxes_kernel(tiles, out):
    for half in range(2):
        rows = []
        for k in range(half * 8, half * 8 + 8):
            source = (((k >> 1) & 1) * 4 + (k >> 2)) * 2 + (k & 1)
            tile = tiles[pl.ds(source * 8, 8), :]
            rows += [tile, pltpu.roll(tile, 64, 1)]
        turned = jnp.transpose(jnp.concatenate(rows, axis=0))
        out[:, half * LANES : (half + 1) * LANES] = turned[:64]


def in_vmem():
    return pl.BlockSpec(memory_space=pltpu.VMEM)


def budget(mib):
    return pltpu.CompilerParams(vmem_limit_bytes=mib * 2**20)


def partials(slot_elems, slot_tiles, source_field, weights):
    outside = pl.BlockSpec(memory_space=pltpu.HBM)
    return pl.pallas_call(
        partials_kernel,
        out_shape=jax.ShapeDtypeStruct((PEERS * CHUNK, LANES), jnp.float32),
        in_specs=[outside] * 4,
        out_specs=in_vmem(),
        scratch_shapes=[
            pltpu.VMEM((8192, LANES), jnp.float32),
            pltpu.VMEM((128, 2, 16, LANES), jnp.bfloat16),
            pltpu.VMEM((136, LANES), jnp.int32),
            pltpu.VMEM((1024, 1024), jnp.bfloat16),
            pltpu.VMEM((128, 16, 256), jnp.bfloat16),
            pltpu.VMEM((16, 128), jnp.int32),
            pltpu.SMEM((16, 128), jnp.int32),
            pltpu.SMEM((128,), jnp.int32),
            pltpu.SMEM((RESIDUES,), jnp.int32),
            pltpu.SemaphoreType.DMA((PIECES + 4,)),
        ],
        compiler_params=budget(53),
        name="partials",
    )(
        pltpu.with_memory_space_constraint(slot_elems, pltpu.HBM),
        pltpu.with_memory_space_constraint(slot_tiles, pltpu.HBM),
        source_field,
        weights,
    )


def bins(arrived):
    return pl.pallas_call(
        bins_kernel,
        out_shape=[jax.ShapeDtypeStruct((rows, LANES), jnp.float32) for rows in (128, 128, 64)],
        in_specs=[in_vmem()],
        out_specs=[in_vmem()] * 3,
        compiler_params=budget(8),
        name="bins",
    )(arrived)


def boxes(tiles):
    return pl.pallas_call(
        boxes_kernel,
        out_shape=jax.ShapeDtypeStruct((64, 256), jnp.float32),
        in_specs=[in_vmem()],
        out_specs=in_vmem(),
        compiler_params=budget(4),
        name="boxes",
    )(tiles)


def ahead(block, distance):
    size = lax.axis_size("curve")
    return lax.ppermute(block, "curve", [(i, (i + distance) % size) for i in range(size)])


def exchange(messages, groups):
    return lax.all_to_all(
        messages,
        ("curve", "lev"),
        split_axis=0,
        concat_axis=0,
        tiled=True,
        axis_index_groups=groups,
    )


def per_device(source_field, slot_elems, slot_tiles, weights):
    lev_size = lax.axis_size("lev")
    blocks = range(lax.axis_size("curve") // 2)
    pairs = [[k * 2 * lev_size + m for m in range(2 * lev_size)] for k in blocks]
    sending = partials(slot_elems, slot_tiles, source_field, weights)
    arrived = exchange(sending.reshape(PEERS, 1, CHUNK * LANES), pairs)
    own, second, third = bins(arrived.reshape(PEERS * CHUNK, LANES))
    third = ahead(third, 4)
    total = own + ahead(second, 2)
    total = total + jnp.pad(third, ((0, 64), (0, 0)))
    holders = [
        [(2 * k + i) * lev_size + CLASSES * a + c for i in range(2) for a in range(4)]
        for k in blocks
        for c in range(CLASSES)
    ]
    mine = exchange(total.reshape(8, 16, LANES), holders)
    return boxes(mine.reshape(LANES, LANES))


def solution(mesh):
    placed = (
        P(("curve", "lev"), None),
        P(None, ("curve", "lev")),
        P(("curve", "lev")),
        P(("curve", "lev"), None, None),
    )
    return jax.shard_map(
        per_device, mesh=mesh, in_specs=placed, out_specs=P(None, ("curve", "lev")), check_vma=False
    )
```
